32 devices in a mesh: dp: 2 (over core), fsdp: 16 (over z, y, x).
Axes of the slice: x: 2, y: 2, z: 4, core: 2. Of those that a mesh axis runs over, the one named last changes fastest.
Arguments:
- tokens: bfloat16 [8192, 4096], P(('dp', 'fsdp')), may hold values from -6 to 6
- block_codes: bfloat16 [256, 128, 128], P('fsdp'), may hold values from -4 to 4
- scales: float32 [256], P('fsdp'), may hold values from 0.008 to 0.03
- counts: int32 [16], replicated, may hold values from 0 to 16, as said below
- cotangent: bfloat16 [8192, 512], P(('dp', 'fsdp')), may hold values from -6 to 6
Outputs:
- projected: bfloat16 [8192, 512], P(('dp', 'fsdp'))
- token_grad: bfloat16 [8192, 4096], P(('dp', 'fsdp'))
- block_grad: bfloat16 [256, 128, 128], P('fsdp')
The draws below stay inside these ranges and needn't reach their ends.
Inputs may be any that keep to these rules, and one draw needn't show every extreme that they name: counts sum to 128; each is at most 16, and some owner has exactly 16 and some none; slots past an owner's count hold values that are not used.
All inputs are finite; a program needn't handle non-finite values.
Results may differ from the reference program's by a relative error of at most 0.009.
Values may be sent and summed in bfloat16 or wider, within the bound.
No kernel may reach another device: no remote copies, remote signals or barrier semaphores. Data moves between devices by JAX's collectives and lax.ppermute only.
A program may use at most 128 MiB of HBM per device.

```python
import math
import jax
import jax.numpy as jnp
from jax import lax

D = 4096
KC = 512
TILE = 128
TOKENS = 8192
NBLK = 128
MEAN = 8
MOST = 16
N_FSDP = 16


def draw_counts(key, part):
    shuffled = jax.random.permutation(jax.random.fold_in(key, 11), N_FSDP)
    amounts = jax.random.randint(jax.random.fold_in(key, 12), (N_FSDP // 2,), 0, MEAN + 1)
    amounts = amounts.at[0].set(MEAN)
    shifts = jnp.zeros((N_FSDP,), jnp.int32)
    shifts = shifts.at[shuffled[0::2]].set(amounts).at[shuffled[1::2]].set(-amounts)
    return (MEAN + shifts).astype(jnp.int32)


def strengthened(values, own_key, source, target, blocks, factor):
    owner, partner = [(jnp.arange(values.shape[dim]) // (values.shape[dim] // blocks)).reshape([-1 if axis == dim else 1 for axis in range(values.ndim)]) for dim in (source, target)]
    chosen = jax.random.permutation(own_key, blocks)[partner]
    strong = (owner == chosen) | (owner == (partner + blocks // 2) % blocks)
    return jnp.where(strong, factor * values, values)


def steps_of(own_key, shape, split, low, high):
    loudness = 1.0
    for dim, parts in split:
        steps = jax.random.uniform(jax.random.fold_in(jax.random.fold_in(own_key, 6), dim), (parts,), jnp.float32, low / len(split), high / len(split))
        loudness = loudness * jnp.repeat(jnp.exp(steps), shape[dim] // parts).reshape((-1,) + (1,) * (len(shape) - 1 - dim))
    return loudness


def normal_values(own_key, shape, scale, most, cuts=(), held_as=jnp.bfloat16):
    loudness = steps_of(own_key, shape, cuts, -0.22, 0.18) if cuts else 1.0
    values = jax.random.normal(own_key, shape, jnp.float32) * scale * loudness
    return jnp.minimum(jnp.maximum(values, -most), most).astype(held_as)


def heavy_noise(stream_key, extent, width, limit, cuts, heavy, kind=jnp.bfloat16):
    values = width * jax.random.normal(stream_key, extent, jnp.float32)
    if cuts:
        values = values * steps_of(stream_key, extent, cuts, -0.22, 0.18)
    return jnp.clip(strengthened(values, jax.random.fold_in(stream_key, 3), *heavy), -limit, limit).astype(kind)


def setup_inputs(seed: int = 0) -> dict:
    arg_keys = jax.random.split(jax.random.key(seed), 6)
    tokens = heavy_noise(arg_keys[0], (TOKENS, D), 1.0, 6.0, ((0, 32),), (0, 1, 32, 2.75))
    block_codes = normal_values(arg_keys[1], (N_FSDP * MOST, TILE, TILE), 1.0, 4.0, ((0, 16),))
    scales = jnp.clip(jnp.exp(math.log(0.03) - 1.3217558 * jax.random.uniform(arg_keys[2], (N_FSDP * MOST,), jnp.float32) ** steps_of(arg_keys[2], (N_FSDP * MOST,), ((0, 16),), -0.2, 0.2)), 0.008, 0.03)
    counts = draw_counts(jax.random.fold_in(arg_keys[5], 71), 0)
    cotangent = normal_values(arg_keys[4], (TOKENS, KC), 1.0, 6.0, ((0, 32),))
    return {"tokens": tokens, "block_codes": block_codes, "scales": scales, "counts": counts, "cotangent": cotangent}


def block_index(counts):
    run_ends = jnp.cumsum(counts).astype(jnp.int32)
    offsets = (run_ends - counts).astype(jnp.int32)
    block_ids = jnp.arange(NBLK, dtype=jnp.int32)
    owners = lax.optimization_barrier(jnp.sum((run_ends[None, :] <= block_ids[:, None]).astype(jnp.int32), axis=1))
    matched = owners[:, None] == jnp.arange(N_FSDP, dtype=jnp.int32)[None, :]
    run_start = lax.optimization_barrier(jnp.sum(jnp.where(matched, offsets[None, :], 0), axis=1)).astype(jnp.int32)
    source_ids = (owners * MOST + block_ids - run_start).astype(jnp.int32)
    return (offsets, source_ids)

def reference(tokens, block_codes, scales, counts, cotangent):
    offsets, source_ids = block_index(counts)
    blocks = block_codes[source_ids].astype(jnp.float32) * scales[source_ids][:, None, None]
    blocks = blocks.astype(jnp.bfloat16)
    weight = blocks.reshape(D // TILE, KC // TILE, TILE, TILE).transpose(0, 2, 1, 3).reshape(D, KC)
    projected = jnp.dot(tokens, weight, preferred_element_type=jnp.float32).astype(jnp.bfloat16)
    token_grad = jnp.dot(cotangent, weight.T, preferred_element_type=jnp.float32).astype(jnp.bfloat16)
    grad = jnp.dot(tokens.T, cotangent, preferred_element_type=jnp.float32) * (1.0 / math.sqrt(TOKENS))
    grad_blocks = grad.reshape(D // TILE, TILE, KC // TILE, TILE).transpose(0, 2, 1, 3).reshape(NBLK, TILE, TILE)
    slot_ids = jnp.arange(N_FSDP * MOST, dtype=jnp.int32)
    owner_of = slot_ids // MOST
    within = slot_ids % MOST
    wanted = (offsets[owner_of] + within).astype(jnp.int32)
    is_valid = within < counts[owner_of]
    picked = grad_blocks[jnp.clip(wanted, 0, NBLK - 1)]
    block_grad = jnp.where(is_valid[:, None, None], picked, jnp.float32(0.0)).astype(jnp.bfloat16)
    return (projected, token_grad, block_grad)
```

```python
import functools
import math

import jax
import jax.numpy as jnp
from jax import lax
from jax.experimental import pallas as pl
from jax.experimental.pallas import tpu as pltpu
from jax.sharding import PartitionSpec as P


PERIOD = 8
INNER = 4
VMEM = pltpu.VMEM
BF16 = jnp.bfloat16


def class_of(core, place):
    return (place // 2) * 4 + core * 2 + place % 2


def prefix(counts, stop):
    return lax.fori_loop(0, stop, lambda i, total: total + counts[i], jnp.int32(0))


def lead(cls, start):
    return (cls - start) & (PERIOD - 1)


def here():
    me = lax.axis_index("fsdp")
    return lax.axis_index("dp"), me // INNER, me % INNER, me


def spread_kernel(slots, reach, counts, scales, codes, *outs):
    core, _, place, me = here()
    start = prefix(counts, me)
    for step, out in enumerate(outs):
        first = lead(class_of(core, place ^ step), start)
        for t in range(reach):
            slot = jnp.minimum(first + PERIOD * t, slots - 1)
            out[t] = (codes[slot].astype(jnp.float32) * scales[slot]).astype(BF16)


def stack_kernel(reach, *refs):
    out = refs[-1]
    for m, ref in enumerate(refs[:-1]):
        out[pl.ds(m * reach, reach)] = ref[...]


def class_kernel(planes, reach, counts, *refs):
    ins, out, starts = refs[:planes], refs[planes], refs[planes + 1]
    core, plane, place, _ = here()
    cls = class_of(core, place)

    def note(i, total):
        starts[i] = total
        return total + counts[i]

    lax.fori_loop(0, planes * INNER, note, jnp.int32(0))
    for shift, ref in enumerate(ins):
        source = lax.rem(plane + planes - shift, planes)
        for m in range(INNER):
            owner = source * INNER + (place ^ m)
            first = lead(cls, starts[owner])
            for t in range(reach):

                @pl.when(first + PERIOD * t < counts[owner])
                def _(first=first, owner=owner, t=t, m=m, ref=ref):
                    out[(starts[owner] + first) // PERIOD + t] = ref[m * reach + t]


def grad_kernel(scale, tile, per_step, mine, theirs, cot_mine, cot_theirs, *refs):
    outs, quad = refs[:INNER], refs[INNER]
    core, _, place, _ = here()
    half = cot_mine.shape[1] // 2
    columns = pl.ds(pl.multiple_of(core * half, half), half)
    left, right = cot_mine[:, columns], cot_theirs[:, columns]
    for k in range(per_step):
        rows = pl.ds(2 * tile * k, 2 * tile)
        dims = (((0,), (0,)), ((), ()))
        part = lax.dot_general(mine[:, rows], left, dims, preferred_element_type=jnp.float32)
        part += lax.dot_general(theirs[:, rows], right, dims, preferred_element_type=jnp.float32)
        quad[...] = part * scale
        for m, out in enumerate(outs):
            where = place ^ m
            row = pl.multiple_of((where // 2) * tile, tile)
            col = pl.multiple_of((where % 2) * tile, tile)
            out[k] = quad[pl.ds(row, tile), pl.ds(col, tile)].astype(BF16)


def window(counts, cls, plane, blocks, span):
    start = prefix(counts, plane * INNER)
    return jnp.minimum((start + lead(cls, start)) // PERIOD, blocks - span)


def plane_sum_kernel(planes, span, counts, *refs):
    ins, outs, total = refs[:INNER], refs[INNER:-1], refs[-1]
    core, plane, place, _ = here()
    cls = class_of(core, place)
    blocks = total.shape[0]
    for j in range(blocks):
        acc = ins[0][j].astype(jnp.float32)
        for ref in ins[1:]:
            acc += ref[j].astype(jnp.float32)
        total[j] = acc.astype(BF16)
    for shift, out in enumerate(outs):
        target = lax.rem(plane + shift, planes)
        out[...] = total[pl.ds(window(counts, cls, target, blocks, span), span)]


def owner_kernel(blocks, reach, span, planes, counts, *refs):
    ins, outs, total = refs[:planes], refs[planes:-1], refs[-1]
    core, plane, place, _ = here()
    cls = class_of(core, place)
    acc = ins[0][...].astype(jnp.float32)
    for ref in ins[1:]:
        acc += ref[...].astype(jnp.float32)
    total[...] = acc.astype(BF16)
    base = window(counts, cls, plane, blocks, span)
    for m, out in enumerate(outs):
        start = prefix(counts, plane * INNER + (place ^ m))
        j = (start + lead(cls, start)) // PERIOD - base
        for t in range(reach):
            out[t] = total[jnp.clip(j + t, 0, span - 1)]


def slots_kernel(slots, reach, counts, *refs):
    ins, out = refs[:-1], refs[-1]
    core, _, place, me = here()
    start, count = prefix(counts, me), counts[me]
    for n, ref in enumerate(ins):
        side = core ^ (n // INNER)
        first = lead(class_of(side, place ^ (n % INNER)), start)
        for t in range(reach):
            slot = first + PERIOD * t

            @pl.when(slot < slots)
            def _(slot=slot, ref=ref, t=t):
                value = ref[t]
                out[slot] = jnp.where(slot < count, value, jnp.zeros_like(value))


def product_kernel(tile, per_step, tokens, cot, *refs):
    pieces, projected, token_grad, weight, acc = refs[:-4], refs[-4], refs[-3], refs[-2], refs[-1]
    core, _, place, _ = here()
    step = pl.program_id(0)
    for n, ref in enumerate(pieces):
        side, where = core ^ (n // INNER), place ^ (n % INNER)
        col = pl.multiple_of((side * 2 + where % 2) * tile, tile)
        for k in range(per_step):
            row = pl.multiple_of((where // 2) * tile + 2 * tile * k, tile)
            weight[pl.ds(row, tile), pl.ds(col, tile)] = ref[k]

    @pl.when(step == 0)
    def _():
        acc[...] = jnp.zeros_like(acc)

    acc[...] += jnp.dot(tokens[...], weight[...], preferred_element_type=jnp.float32)
    token_grad[...] = lax.dot_general(
        cot[...], weight[...], (((1,), (1,)), ((), ())), preferred_element_type=jnp.float32
    ).astype(BF16)

    @pl.when(step == pl.num_programs(0) - 1)
    def _():
        projected[...] = acc[...].astype(BF16)


def whole():
    return pl.BlockSpec(memory_space=VMEM)


def scalars():
    return pl.BlockSpec(memory_space=pltpu.SMEM)


def room(mebibytes):
    return pltpu.CompilerParams(vmem_limit_bytes=mebibytes * 2**20)


def cost(flops, nbytes):
    return pl.CostEstimate(flops=flops, bytes_accessed=nbytes, transcendentals=0)


def body(tokens, block_codes, scales, counts, cotangent):
    owners = lax.axis_size("fsdp")
    planes = owners // INNER
    slots, tile = block_codes.shape[:2]
    rows, width = tokens.shape
    key_width = cotangent.shape[1]
    blocks = (width // tile) * (key_width // tile) // PERIOD
    reach = -(-slots // PERIOD)
    span = min(-(-slots * INNER // PERIOD), blocks)
    total_tokens = rows * lax.axis_size("dp") * owners

    def many(n):
        return jax.ShapeDtypeStruct((n, tile, tile), BF16)

    block_bytes = tile * tile * 2

    def beside(value, m):
        return lax.ppermute(value, "fsdp", [(i, i ^ m) for i in range(owners)])

    def along(value, shift):
        pairs = [(i, (i + shift * INNER) % owners) for i in range(owners)]
        return lax.ppermute(value, "fsdp", pairs)

    def across(value):
        return lax.ppermute(value, "dp", [(0, 1), (1, 0)])

    def call(kernel, *operands, **how):
        return pl.pallas_call(kernel, **how)(*operands)

    their_tokens, their_cot = across(tokens), across(cotangent)

    spread = call(
        functools.partial(spread_kernel, slots, reach),
        counts, scales, block_codes,
        out_shape=[many(reach)] * INNER,
        in_specs=[scalars(), scalars(), whole()],
        out_specs=[whole()] * INNER,
        cost_estimate=cost(8 * block_bytes, 24 * block_bytes),
        compiler_params=room(8),
    )
    near = [spread[0]] + [beside(spread[m], m) for m in range(1, INNER)]

    per_step = 4
    steps = blocks // per_step
    wide = 2 * tile * per_step
    grads = call(
        functools.partial(grad_kernel, 1.0 / math.sqrt(total_tokens), tile, per_step),
        tokens, their_tokens, cotangent, their_cot,
        out_shape=[many(blocks)] * INNER,
        grid=(steps,),
        in_specs=[pl.BlockSpec((rows, wide), lambda i: (0, i))] * 2
        + [pl.BlockSpec((rows, key_width), lambda i: (0, 0))] * 2,
        out_specs=[pl.BlockSpec((per_step, tile, tile), lambda i: (i, 0, 0))] * INNER,
        scratch_shapes=[VMEM((2 * tile, 2 * tile), jnp.float32)],
        cost_estimate=cost(2 * rows * width * key_width, 6 * rows * width),
        compiler_params=room(20),
    )
    parts = [grads[0]] + [beside(grads[m], m) for m in range(1, INNER)]

    stacked = call(
        functools.partial(stack_kernel, reach),
        *near,
        out_shape=many(INNER * reach),
        in_specs=[whole()] * INNER,
        out_specs=whole(),
        cost_estimate=cost(8 * block_bytes, 16 * block_bytes),
        compiler_params=room(8),
    )
    held = [stacked] + [along(stacked, s) for s in range(1, planes)]

    own_class = call(
        functools.partial(class_kernel, planes, reach),
        counts, *held,
        out_shape=many(blocks),
        in_specs=[scalars()] + [whole()] * planes,
        out_specs=whole(),
        scratch_shapes=[pltpu.SMEM((owners,), jnp.int32)],
        cost_estimate=cost(32 * block_bytes, 48 * block_bytes),
        compiler_params=room(8),
    )
    classes = [own_class] + [beside(own_class, m) for m in range(1, INNER)]

    windows = call(
        functools.partial(plane_sum_kernel, planes, span),
        counts, *parts,
        out_shape=[many(span)] * planes,
        in_specs=[scalars()] + [whole()] * INNER,
        out_specs=[whole()] * planes,
        scratch_shapes=[VMEM((blocks, tile, tile), BF16)],
        cost_estimate=cost(64 * block_bytes, 96 * block_bytes),
        compiler_params=room(12),
    )
    sums = [windows[0]] + [along(windows[s], s) for s in range(1, planes)]

    sent = call(
        functools.partial(owner_kernel, blocks, reach, span, planes),
        counts, *sums,
        out_shape=[many(reach)] * INNER,
        in_specs=[scalars()] + [whole()] * planes,
        out_specs=[whole()] * INNER,
        scratch_shapes=[VMEM((span, tile, tile), BF16)],
        cost_estimate=cost(32 * block_bytes, 48 * block_bytes),
        compiler_params=room(8),
    )
    mine = [sent[0]] + [beside(sent[m], m) for m in range(1, INNER)]

    all_classes = classes + [across(own_class)] + [across(c) for c in classes[1:]]
    projected, token_grad = call(
        functools.partial(product_kernel, tile, per_step),
        tokens, cotangent, *all_classes,
        out_shape=[
            jax.ShapeDtypeStruct((rows, key_width), BF16),
            jax.ShapeDtypeStruct((rows, width), BF16),
        ],
        grid=(steps,),
        in_specs=[
            pl.BlockSpec((rows, wide), lambda i: (0, i)),
            pl.BlockSpec((rows, key_width), lambda i: (0, 0)),
        ]
        + [pl.BlockSpec((per_step, tile, tile), lambda i: (i, 0, 0))] * (2 * INNER),
        out_specs=[
            pl.BlockSpec((rows, key_width), lambda i: (0, 0)),
            pl.BlockSpec((rows, wide), lambda i: (0, i)),
        ],
        scratch_shapes=[VMEM((wide, key_width), BF16), VMEM((rows, key_width), jnp.float32)],
        cost_estimate=cost(4 * rows * width * key_width, 12 * rows * width),
        compiler_params=room(28),
    )

    all_mine = mine + [across(v) for v in mine]
    block_grad = call(
        functools.partial(slots_kernel, slots, reach),
        counts, *all_mine,
        out_shape=many(slots),
        in_specs=[scalars()] + [whole()] * (2 * INNER),
        out_specs=whole(),
        cost_estimate=cost(16 * block_bytes, 32 * block_bytes),
        compiler_params=room(8),
    )
    return (projected, token_grad, block_grad)


def solution(mesh):
    return jax.shard_map(
        body,
        mesh=mesh,
        in_specs=(
            P(("dp", "fsdp"), None),
            P("fsdp", None, None),
            P("fsdp"),
            P(),
            P(("dp", "fsdp"), None),
        ),
        out_specs=(P(("dp", "fsdp"), None), P(("dp", "fsdp"), None), P("fsdp", None, None)),
        check_vma=False,
    )
```

```python
import functools
import math

import jax
import jax.numpy as jnp
from jax import lax
from jax.experimental import pallas as pl
from jax.experimental.pallas import tpu as pltpu
from jax.sharding import PartitionSpec as P


PERIOD = 8
INNER = 4
VMEM = pltpu.VMEM
BF16 = jnp.bfloat16


def class_of(core, place):
    return (place // 2) * 4 + core * 2 + place % 2


def prefix(counts, stop):
    return lax.fori_loop(0, stop, lambda i, total: total + counts[i], jnp.int32(0))


def lead(cls, start):
    return (cls - start) & (PERIOD - 1)


def here():
    me = lax.axis_index("fsdp")
    return lax.axis_index("dp"), me // INNER, me % INNER, me


def spread_kernel(slots, reach, counts_in, scales_in, codes_in, *refs):
    (tokens_in, cot_in), (tokens, cot), outs = refs[:2], refs[2:4], refs[4 : 4 + INNER]
    counts, scales, codes, done, wide_done = refs[4 + INNER :]
    wide_loads = [
        pltpu.make_async_copy(source, target, wide_done.at[n])
        for n, (source, target) in enumerate(((tokens_in, tokens), (cot_in, cot)))
    ]
    loads = [
        pltpu.make_async_copy(source, target, done.at[n])
        for n, (source, target) in enumerate(
            ((counts_in, counts), (scales_in, scales), (codes_in, codes))
        )
    ]
    for load in loads + wide_loads:
        load.start()
    core, _, place, me = here()
    loads[0].wait()
    start = prefix(counts, me)
    loads[1].wait()
    loads[2].wait()
    for step, out in enumerate(outs):
        first = lead(class_of(core, place ^ step), start)
        for t in range(reach):
            slot = jnp.minimum(first + PERIOD * t, slots - 1)
            out[t] = (codes[slot].astype(jnp.float32) * scales[slot]).astype(BF16)
    for load in wide_loads:
        load.wait()


def stack_kernel(reach, *refs):
    out = refs[-1]
    for m, ref in enumerate(refs[:-1]):
        out[pl.ds(m * reach, reach)] = ref[...]


def class_kernel(planes, reach, counts, *refs):
    ins, outs, starts = refs[:planes], refs[planes:-1], refs[-1]
    core, plane, place, _ = here()
    cls = class_of(core, place)
    per_out = outs[0].shape[0]

    def note(i, total):
        starts[i] = total
        return total + counts[i]

    lax.fori_loop(0, planes * INNER, note, jnp.int32(0))
    for shift, ref in enumerate(ins):
        source = plane ^ shift
        for m in range(INNER):
            owner = source * INNER + (place ^ m)
            first = lead(cls, starts[owner])
            for t in range(reach):
                j = (starts[owner] + first) // PERIOD + t
                held = first + PERIOD * t < counts[owner]
                for n, out in enumerate(outs):

                    @pl.when(held & (j // per_out == n))
                    def _(j=j, t=t, m=m, n=n, ref=ref, out=out):
                        out[j - n * per_out] = ref[m * reach + t]


def grad_kernel(scale, tile, chunks, mine, theirs, cot_mine, cot_theirs, *refs):
    outs, quad = refs[:INNER], refs[INNER]
    core, _, place, _ = here()
    half = cot_mine.shape[1] // 2
    columns = pl.ds(pl.multiple_of(core * half, half), half)
    left, right = cot_mine[:, columns], cot_theirs[:, columns]
    wide = mine.shape[1] // chunks
    per_chunk = wide // (2 * tile)
    dims = (((0,), (0,)), ((), ()))

    def chunk(i, carry):
        for k in range(per_chunk):
            rows = pl.ds(pl.multiple_of(i * wide + 2 * tile * k, 2 * tile), 2 * tile)
            part = lax.dot_general(mine[:, rows], left, dims, preferred_element_type=jnp.float32)
            part += lax.dot_general(theirs[:, rows], right, dims, preferred_element_type=jnp.float32)
            quad[k] = part * scale
            for m, out in enumerate(outs):
                where = place ^ m
                row = pl.multiple_of((where // 2) * tile, tile)
                col = pl.multiple_of((where % 2) * tile, tile)
                out[i * per_chunk + k] = quad[k, pl.ds(row, tile), pl.ds(col, tile)].astype(BF16)
        return carry

    lax.fori_loop(0, chunks, chunk, 0)


def window(counts, cls, plane, blocks, span):
    start = prefix(counts, plane * INNER)
    return jnp.minimum((start + lead(cls, start)) // PERIOD, blocks - span)


def plane_sum_kernel(span, counts, *refs):
    ins, outs, total = refs[:INNER], refs[INNER:-1], refs[-1]
    core, plane, place, _ = here()
    cls = class_of(core, place)
    blocks = total.shape[0]
    for j in range(blocks):
        acc = ins[0][j].astype(jnp.float32)
        for ref in ins[1:]:
            acc += ref[j].astype(jnp.float32)
        total[j] = acc.astype(BF16)
    for shift, out in enumerate(outs):
        target = plane ^ shift
        out[...] = total[pl.ds(window(counts, cls, target, blocks, span), span)]


def owner_kernel(blocks, reach, span, planes, counts, *refs):
    ins, outs, total = refs[:planes], refs[planes:-1], refs[-1]
    core, plane, place, _ = here()
    cls = class_of(core, place)
    acc = ins[0][...].astype(jnp.float32)
    for ref in ins[1:]:
        acc += ref[...].astype(jnp.float32)
    total[...] = acc.astype(BF16)
    base = window(counts, cls, plane, blocks, span)
    for m, out in enumerate(outs):
        start = prefix(counts, plane * INNER + (place ^ m))
        j = (start + lead(cls, start)) // PERIOD - base
        for t in range(reach):
            out[t] = total[jnp.clip(j + t, 0, span - 1)]


def slots_kernel(slots, reach, counts, *refs):
    ins, out = refs[:-1], refs[-1]
    core, _, place, me = here()
    start, count = prefix(counts, me), counts[me]
    for n, ref in enumerate(ins):
        side = core ^ (n // INNER)
        first = lead(class_of(side, place ^ (n % INNER)), start)
        for t in range(reach):
            slot = first + PERIOD * t

            @pl.when(slot < slots)
            def _(slot=slot, ref=ref, t=t):
                value = ref[t]
                out[slot] = jnp.where(slot < count, value, jnp.zeros_like(value))


def product_kernel(tile, per_step, last, tokens, cot, *refs):
    pieces, refs = refs[: 2 * INNER], refs[2 * INNER :]
    before = refs[0] if last else None
    projected, token_grad, weight, acc = refs[2:] if last else refs
    core, _, place, _ = here()
    step = pl.program_id(0)
    for n, ref in enumerate(pieces):
        side, where = core ^ (n // INNER), place ^ (n % INNER)
        col = pl.multiple_of((side * 2 + where % 2) * tile, tile)
        for k in range(per_step):
            row = pl.multiple_of((where // 2) * tile + 2 * tile * k, tile)
            weight[pl.ds(row, tile), pl.ds(col, tile)] = ref[k]

    @pl.when(step == 0)
    def _():
        acc[...] = before[...] if last else jnp.zeros_like(acc)

    acc[...] += jnp.dot(tokens[...], weight[...], preferred_element_type=jnp.float32)
    token_grad[...] = lax.dot_general(
        cot[...], weight[...], (((1,), (1,)), ((), ())), preferred_element_type=jnp.float32
    ).astype(BF16)

    @pl.when(step == pl.num_programs(0) - 1)
    def _():
        projected[...] = acc[...].astype(projected.dtype)


def whole():
    return pl.BlockSpec(memory_space=VMEM)


def far():
    return pl.BlockSpec(memory_space=pl.ANY)


def stays(value):
    return pltpu.with_memory_space_constraint(value, pltpu.HBM)


def scalars():
    return pl.BlockSpec(memory_space=pltpu.SMEM)


def room(mebibytes):
    return pltpu.CompilerParams(vmem_limit_bytes=mebibytes * 2**20)


def cost(flops, nbytes):
    return pl.CostEstimate(flops=flops, bytes_accessed=nbytes, transcendentals=0)


def body(tokens, block_codes, scales, counts, cotangent):
    owners = lax.axis_size("fsdp")
    planes = owners // INNER
    slots, tile = block_codes.shape[:2]
    rows, width = tokens.shape
    key_width = cotangent.shape[1]
    blocks = (width // tile) * (key_width // tile) // PERIOD
    reach = -(-slots // PERIOD)
    span = min(-(-slots * INNER // PERIOD), blocks)
    total_tokens = rows * lax.axis_size("dp") * owners

    def many(n):
        return jax.ShapeDtypeStruct((n, tile, tile), BF16)

    block_bytes = tile * tile * 2

    def beside(value, m):
        return lax.ppermute(value, "fsdp", [(i, i ^ m) for i in range(owners)])

    def along(value, shift):
        pairs = [(i, i ^ (shift * INNER)) for i in range(owners)]
        return lax.ppermute(value, "fsdp", pairs)

    def across(value):
        return lax.ppermute(value, "dp", [(0, 1), (1, 0)])

    def call(kernel, *operands, **how):
        return pl.pallas_call(kernel, **how)(*operands)

    their_tokens, their_cot = across(tokens), across(cotangent)

    my_tokens, my_cot, *spread = call(
        functools.partial(spread_kernel, slots, reach),
        stays(counts),
        stays(scales),
        stays(block_codes),
        stays(tokens),
        stays(cotangent),
        out_shape=[
            pltpu.VMEM((rows, width), BF16),
            pltpu.VMEM((rows, key_width), BF16),
        ]
        + [many(reach)] * INNER,
        in_specs=[far()] * 5,
        out_specs=[far()] * 2 + [whole()] * INNER,
        scratch_shapes=[
            pltpu.SMEM((owners,), jnp.int32),
            pltpu.SMEM((slots,), jnp.float32),
            VMEM((slots, tile, tile), BF16),
            pltpu.SemaphoreType.DMA((3,)),
            pltpu.SemaphoreType.DMA((2,)),
        ],
        cost_estimate=cost(8 * block_bytes, 24 * block_bytes),
        compiler_params=room(8),
    )
    near = [spread[0]] + [beside(spread[m], m) for m in range(1, INNER)]

    chunks = 4
    grads = call(
        functools.partial(grad_kernel, 1.0 / math.sqrt(total_tokens), tile, chunks),
        my_tokens,
        their_tokens,
        my_cot,
        their_cot,
        out_shape=[many(blocks)] * INNER,
        in_specs=[whole()] * 4,
        out_specs=[whole()] * INNER,
        scratch_shapes=[
            VMEM((width // (2 * tile * chunks), 2 * tile, 2 * tile), jnp.float32)
        ],
        cost_estimate=cost(2 * rows * width * key_width, 6 * rows * width),
        compiler_params=room(20),
    )
    parts = [grads[0]] + [beside(grads[m], m) for m in range(1, INNER)]

    stacked = call(
        functools.partial(stack_kernel, reach),
        *near,
        out_shape=many(INNER * reach),
        in_specs=[whole()] * INNER,
        out_specs=whole(),
        cost_estimate=cost(8 * block_bytes, 16 * block_bytes),
        compiler_params=room(8),
    )
    held = [stacked] + [along(stacked, s) for s in range(1, planes)]

    own_classes = call(
        functools.partial(class_kernel, planes, reach),
        counts,
        *held,
        out_shape=[many(blocks // 2)] * 2,
        in_specs=[scalars()] + [whole()] * planes,
        out_specs=[whole()] * 2,
        scratch_shapes=[pltpu.SMEM((owners,), jnp.int32)],
        cost_estimate=cost(32 * block_bytes, 48 * block_bytes),
        compiler_params=room(8),
    )

    windows = call(
        functools.partial(plane_sum_kernel, span),
        counts, *parts,
        out_shape=[many(span)] * planes,
        in_specs=[scalars()] + [whole()] * INNER,
        out_specs=[whole()] * planes,
        scratch_shapes=[VMEM((blocks, tile, tile), BF16)],
        cost_estimate=cost(64 * block_bytes, 96 * block_bytes),
        compiler_params=room(12),
    )
    sums = [windows[0]] + [along(windows[s], s) for s in range(1, planes)]

    sent = call(
        functools.partial(owner_kernel, blocks, reach, span, planes),
        counts, *sums,
        out_shape=[many(reach)] * INNER,
        in_specs=[scalars()] + [whole()] * planes,
        out_specs=[whole()] * INNER,
        scratch_shapes=[VMEM((span, tile, tile), BF16)],
        cost_estimate=cost(32 * block_bytes, 48 * block_bytes),
        compiler_params=room(8),
    )
    mine = [sent[0]] + [beside(sent[m], m) for m in range(1, INNER)]

    per_step = min(4, blocks // 2)
    steps = blocks // 2 // per_step
    wide = 2 * tile * per_step

    def products(part, carried):
        last = part == 1
        base = part * steps
        own = own_classes[part]
        plane = [own] + [beside(own, m) for m in range(1, INNER)]
        pieces = plane + [across(c) for c in plane]
        square = pl.BlockSpec((rows, key_width), lambda i: (0, 0))
        stripe = pl.BlockSpec((rows, wide), lambda i: (0, base + i))
        return call(
            functools.partial(product_kernel, tile, per_step, last),
            my_tokens,
            my_cot,
            *pieces,
            *carried,
            out_shape=[
                jax.ShapeDtypeStruct((rows, key_width), BF16 if last else jnp.float32),
                jax.ShapeDtypeStruct((rows, width), BF16),
            ],
            grid=(steps,),
            in_specs=[stripe, square]
            + [pl.BlockSpec((per_step, tile, tile), lambda i: (i, 0, 0))] * (2 * INNER)
            + ([square, pl.BlockSpec(memory_space=pl.ANY)] if last else []),
            out_specs=[square, stripe],
            input_output_aliases={2 * INNER + 3: 1} if last else {},
            scratch_shapes=[VMEM((wide, key_width), BF16), VMEM((rows, key_width), jnp.float32)],
            cost_estimate=cost(2 * rows * width * key_width, 6 * rows * width),
            compiler_params=room(28),
        )

    projected, token_grad = products(1, products(0, ()))

    all_mine = mine + [across(v) for v in mine]
    block_grad = call(
        functools.partial(slots_kernel, slots, reach),
        counts, *all_mine,
        out_shape=many(slots),
        in_specs=[scalars()] + [whole()] * (2 * INNER),
        out_specs=whole(),
        cost_estimate=cost(16 * block_bytes, 32 * block_bytes),
        compiler_params=room(8),
    )
    return (projected, token_grad, block_grad)


def solution(mesh):
    return jax.shard_map(
        body,
        mesh=mesh,
        in_specs=(
            P(("dp", "fsdp"), None),
            P("fsdp", None, None),
            P("fsdp"),
            P(),
            P(("dp", "fsdp"), None),
        ),
        out_specs=(P(("dp", "fsdp"), None), P(("dp", "fsdp"), None), P("fsdp", None, None)),
        check_vma=False,
    )
```

```python
import functools
import math

import jax
import jax.numpy as jnp
from jax import lax
from jax.experimental import pallas as pl
from jax.experimental.pallas import tpu as pltpu
from jax.sharding import PartitionSpec as P


PERIOD = 8
INNER = 4
VMEM = pltpu.VMEM
BF16 = jnp.bfloat16


def class_of(core, place):
    return (place // 2) * 4 + core * 2 + place % 2


def prefix(counts, stop):
    return lax.fori_loop(0, stop, lambda i, total: total + counts[i], jnp.int32(0))


def lead(cls, start):
    return (cls - start) & (PERIOD - 1)


def here():
    me = lax.axis_index("fsdp")
    return lax.axis_index("dp"), me // INNER, me % INNER, me


def spread_kernel(slots, reach, counts_in, scales_in, codes_in, *refs):
    (tokens_in, cot_in), (tokens, cot), outs = refs[:2], refs[2:4], refs[4 : 4 + INNER]
    counts, scales, codes, done, wide_done = refs[4 + INNER :]
    wide_loads = [
        pltpu.make_async_copy(source, target, wide_done.at[n])
        for n, (source, target) in enumerate(((tokens_in, tokens), (cot_in, cot)))
    ]
    loads = [
        pltpu.make_async_copy(source, target, done.at[n])
        for n, (source, target) in enumerate(
            ((counts_in, counts), (scales_in, scales), (codes_in, codes))
        )
    ]
    for load in loads + wide_loads:
        load.start()
    core, _, place, me = here()
    loads[0].wait()
    start = prefix(counts, me)
    loads[1].wait()
    loads[2].wait()
    for step, out in enumerate(outs):
        first = lead(class_of(core, place ^ step), start)
        for t in range(reach):
            slot = jnp.minimum(first + PERIOD * t, slots - 1)
            out[t] = (codes[slot].astype(jnp.float32) * scales[slot]).astype(BF16)
    for load in wide_loads:
        load.wait()


def stack_kernel(reach, *refs):
    out = refs[-1]
    for m, ref in enumerate(refs[:-1]):
        out[pl.ds(m * reach, reach)] = ref[...]


def class_kernel(planes, reach, counts, *refs):
    ins, outs, starts = refs[:planes], refs[planes:-1], refs[-1]
    core, plane, place, _ = here()
    cls = class_of(core, place)
    per_out = outs[0].shape[0]

    def note(i, total):
        starts[i] = total
        return total + counts[i]

    lax.fori_loop(0, planes * INNER, note, jnp.int32(0))
    for shift, ref in enumerate(ins):
        source = plane ^ shift
        for m in range(INNER):
            owner = source * INNER + (place ^ m)
            first = lead(cls, starts[owner])
            for t in range(reach):
                j = (starts[owner] + first) // PERIOD + t
                held = first + PERIOD * t < counts[owner]
                for n, out in enumerate(outs):

                    @pl.when(held & (j // per_out == n))
                    def _(j=j, t=t, m=m, n=n, ref=ref, out=out):
                        out[j - n * per_out] = ref[m * reach + t]


def grad_kernel(scale, tile, chunks, mine, theirs, cot_mine, cot_theirs, own, *refs):
    outs, quad = refs[:-1], refs[-1]
    core, _, place, _ = here()
    half = cot_mine.shape[1] // 2
    columns = pl.ds(pl.multiple_of(core * half, half), half)
    left, right = cot_mine[:, columns], cot_theirs[:, columns]
    wide = mine.shape[1] // chunks
    per_chunk = wide // (2 * tile)
    dims = (((0,), (0,)), ((), ()))

    def chunk(part, i, carry):
        base = i * per_chunk - part * (chunks // 2) * per_chunk
        for k in range(per_chunk):
            rows = pl.ds(pl.multiple_of(i * wide + 2 * tile * k, 2 * tile), 2 * tile)
            value = lax.dot_general(mine[:, rows], left, dims, preferred_element_type=jnp.float32)
            value += lax.dot_general(
                theirs[:, rows], right, dims, preferred_element_type=jnp.float32
            )
            quad[k] = value * scale
            for m in range(INNER):
                where = place ^ m
                row = pl.multiple_of((where // 2) * tile, tile)
                col = pl.multiple_of((where % 2) * tile, tile)
                block = quad[k, pl.ds(row, tile), pl.ds(col, tile)].astype(BF16)
                if m:
                    outs[2 * (m - 1) + part][base + k] = block
                else:
                    own[i * per_chunk + k] = block
        return carry

    for part in range(2):
        first = part * (chunks // 2)
        lax.fori_loop(first, first + chunks // 2, functools.partial(chunk, part), 0)


def fold_kernel(*refs):
    ins, outs = refs[:4], refs[4:]
    for n, out in enumerate(outs):
        value = ins[2 * n][...].astype(jnp.float32) + ins[2 * n + 1][...].astype(jnp.float32)
        out[...] = value.astype(BF16)


def window(counts, cls, plane, blocks, span):
    start = prefix(counts, plane * INNER)
    return jnp.minimum((start + lead(cls, start)) // PERIOD, blocks - span)


def plane_sum_kernel(span, counts, own, *refs):
    ins, outs, total = refs[:4], refs[4:-1], refs[-1]
    core, plane, place, _ = here()
    cls = class_of(core, place)
    blocks = total.shape[0]
    for j in range(blocks):
        part, row = divmod(j, blocks // 2)
        acc = own[j].astype(jnp.float32)
        for ref in ins[2 * part : 2 * part + 2]:
            acc += ref[row].astype(jnp.float32)
        total[j] = acc.astype(BF16)
    for shift, out in enumerate(outs):
        target = plane ^ shift
        out[...] = total[pl.ds(window(counts, cls, target, blocks, span), span)]


def owner_kernel(blocks, reach, span, planes, counts, *refs):
    ins, outs, total = refs[:planes], refs[planes:-1], refs[-1]
    core, plane, place, _ = here()
    cls = class_of(core, place)
    acc = ins[0][...].astype(jnp.float32)
    for ref in ins[1:]:
        acc += ref[...].astype(jnp.float32)
    total[...] = acc.astype(BF16)
    base = window(counts, cls, plane, blocks, span)
    for m, out in enumerate(outs):
        start = prefix(counts, plane * INNER + (place ^ m))
        j = (start + lead(cls, start)) // PERIOD - base
        for t in range(reach):
            out[t] = total[jnp.clip(j + t, 0, span - 1)]


def slots_kernel(slots, reach, counts, *refs):
    ins, out = refs[:-1], refs[-1]
    core, _, place, me = here()
    start, count = prefix(counts, me), counts[me]
    for n, ref in enumerate(ins):
        side = core ^ (n // INNER)
        first = lead(class_of(side, place ^ (n % INNER)), start)
        for t in range(reach):
            slot = first + PERIOD * t

            @pl.when(slot < slots)
            def _(slot=slot, ref=ref, t=t):
                value = ref[t]
                out[slot] = jnp.where(slot < count, value, jnp.zeros_like(value))


def product_kernel(tile, part, tokens, cot, *refs):
    pieces, refs = refs[:8], refs[8:]
    before, refs = (refs[0], refs[2:]) if part else (None, refs)
    projected, token_grad, left, weight, acc, stripes, done = refs
    core, _, place, _ = here()
    parity = (place // 2) ^ part
    per_piece = pieces[0].shape[0]
    group = left.shape[1] // tile
    stores = []
    for start in range(0, 2 * per_piece, group):
        half, first = divmod(start, per_piece)
        for k in range(group):
            lane = pl.multiple_of((2 * (start + k) + parity) * tile, tile)
            left[:, pl.ds(k * tile, tile)] = tokens[:, pl.ds(lane, tile)]
            for n in range(4):
                side, m = divmod(n, 2)
                col = pl.multiple_of(((core ^ side) * 2 + (place ^ m) % 2) * tile, tile)
                weight[pl.ds(k * tile, tile), pl.ds(col, tile)] = pieces[2 * n + half][first + k]
        value = jnp.dot(left[...], weight[...], preferred_element_type=jnp.float32)
        if start:
            acc[...] += value
        else:
            acc[...] = before[...] + value if part else value
        grads = lax.dot_general(
            cot[...], weight[...], (((1,), (1,)), ((), ())), preferred_element_type=jnp.float32
        ).astype(BF16)
        for k in range(group):
            j = start + k
            stripes[j] = grads[:, k * tile : (k + 1) * tile]
            lane = pl.multiple_of((2 * j + parity) * tile, tile)
            store = pltpu.make_async_copy(
                stripes.at[j], token_grad.at[:, pl.ds(lane, tile)], done.at[j]
            )
            store.start()
            stores.append(store)
    projected[...] = acc[...].astype(projected.dtype)
    for store in stores:
        store.wait()


def whole():
    return pl.BlockSpec(memory_space=VMEM)


def far():
    return pl.BlockSpec(memory_space=pl.ANY)


def stays(value):
    return pltpu.with_memory_space_constraint(value, pltpu.HBM)


def scalars():
    return pl.BlockSpec(memory_space=pltpu.SMEM)


def room(mebibytes):
    return pltpu.CompilerParams(vmem_limit_bytes=mebibytes * 2**20)


def cost(flops, nbytes):
    return pl.CostEstimate(flops=flops, bytes_accessed=nbytes, transcendentals=0)


def body(tokens, block_codes, scales, counts, cotangent):
    owners = lax.axis_size("fsdp")
    planes = owners // INNER
    slots, tile = block_codes.shape[:2]
    rows, width = tokens.shape
    key_width = cotangent.shape[1]
    blocks = (width // tile) * (key_width // tile) // PERIOD
    reach = -(-slots // PERIOD)
    span = min(-(-slots * INNER // PERIOD), blocks)
    total_tokens = rows * lax.axis_size("dp") * owners

    def many(n):
        return jax.ShapeDtypeStruct((n, tile, tile), BF16)

    block_bytes = tile * tile * 2

    def beside(value, m):
        return lax.ppermute(value, "fsdp", [(i, i ^ m) for i in range(owners)])

    def along(value, shift):
        pairs = [(i, i ^ (shift * INNER)) for i in range(owners)]
        return lax.ppermute(value, "fsdp", pairs)

    def across(value):
        return lax.ppermute(value, "dp", [(0, 1), (1, 0)])

    def call(kernel, *operands, **how):
        return pl.pallas_call(kernel, **how)(*operands)

    their_tokens, their_cot = across(tokens), across(cotangent)

    my_tokens, my_cot, *spread = call(
        functools.partial(spread_kernel, slots, reach),
        stays(counts),
        stays(scales),
        stays(block_codes),
        stays(tokens),
        stays(cotangent),
        out_shape=[
            pltpu.VMEM((rows, width), BF16),
            pltpu.VMEM((rows, key_width), BF16),
        ]
        + [many(reach)] * INNER,
        in_specs=[far()] * 5,
        out_specs=[far()] * 2 + [whole()] * INNER,
        scratch_shapes=[
            pltpu.SMEM((owners,), jnp.int32),
            pltpu.SMEM((slots,), jnp.float32),
            VMEM((slots, tile, tile), BF16),
            pltpu.SemaphoreType.DMA((3,)),
            pltpu.SemaphoreType.DMA((2,)),
        ],
        cost_estimate=cost(8 * block_bytes, 24 * block_bytes),
        compiler_params=room(8),
    )
    near = [spread[0]] + [beside(spread[m], m) for m in range(1, INNER)]

    chunks = 4
    half = many(blocks // 2)
    grads = call(
        functools.partial(grad_kernel, 1.0 / math.sqrt(total_tokens), tile, chunks),
        my_tokens,
        their_tokens,
        my_cot,
        their_cot,
        out_shape=[many(blocks)] + [half] * 6,
        in_specs=[whole()] * 4,
        out_specs=[whole()] * 7,
        scratch_shapes=[
            VMEM((width // (2 * tile * chunks), 2 * tile, 2 * tile), jnp.float32)
        ],
        cost_estimate=cost(2 * rows * width * key_width, 6 * rows * width),
        compiler_params=room(20),
    )
    own_part, x_low, x_high, y_low, y_high, far_low, far_high = grads
    folded = call(
        fold_kernel,
        y_low,
        beside(far_low, 1),
        x_high,
        beside(far_high, 2),
        out_shape=[half] * 2,
        in_specs=[whole()] * 4,
        out_specs=[whole()] * 2,
        cost_estimate=cost(16 * block_bytes, 48 * block_bytes),
        compiler_params=room(8),
    )
    parts = [
        own_part,
        beside(x_low, 1),
        beside(folded[0], 2),
        beside(folded[1], 1),
        beside(y_high, 2),
    ]

    stacked = call(
        functools.partial(stack_kernel, reach),
        *near,
        out_shape=many(INNER * reach),
        in_specs=[whole()] * INNER,
        out_specs=whole(),
        cost_estimate=cost(8 * block_bytes, 16 * block_bytes),
        compiler_params=room(8),
    )
    held = [stacked] + [along(stacked, s) for s in range(1, planes) if (s, planes) != (2, 4)]
    if planes == 4:
        held.insert(2, along(held[2], 1))

    own_classes = call(
        functools.partial(class_kernel, planes, reach),
        counts,
        *held,
        out_shape=[many(blocks // 2)] * 2,
        in_specs=[scalars()] + [whole()] * planes,
        out_specs=[whole()] * 2,
        scratch_shapes=[pltpu.SMEM((owners,), jnp.int32)],
        cost_estimate=cost(32 * block_bytes, 48 * block_bytes),
        compiler_params=room(8),
    )

    windows = call(
        functools.partial(plane_sum_kernel, span),
        counts, *parts,
        out_shape=[many(span)] * planes,
        in_specs=[scalars()] + [whole()] * 5,
        out_specs=[whole()] * planes,
        scratch_shapes=[VMEM((blocks, tile, tile), BF16)],
        cost_estimate=cost(64 * block_bytes, 96 * block_bytes),
        compiler_params=room(12),
    )
    sums = [windows[0]] + [along(windows[s], s) for s in range(1, planes)]

    sent = call(
        functools.partial(owner_kernel, blocks, reach, span, planes),
        counts, *sums,
        out_shape=[many(reach)] * INNER,
        in_specs=[scalars()] + [whole()] * planes,
        out_specs=[whole()] * INNER,
        scratch_shapes=[VMEM((span, tile, tile), BF16)],
        cost_estimate=cost(32 * block_bytes, 48 * block_bytes),
        compiler_params=room(8),
    )
    mine = [sent[0]] + [beside(sent[m], m) for m in range(1, INNER)]

    low, high = own_classes
    from_x = [beside(low, 1), beside(high, 1)]
    from_y = [beside(low, 2), beside(high, 2)]
    from_far = [beside(from_x[0], 2), beside(from_y[1], 1)]
    group = min(4, blocks // 2)

    def products(part, own, carried):
        held_by_both = own + [across(c) for c in own]
        return call(
            functools.partial(product_kernel, tile, part),
            my_tokens,
            my_cot,
            *held_by_both,
            *carried,
            out_shape=[
                jax.ShapeDtypeStruct((rows, key_width), BF16 if part else jnp.float32),
                pltpu.HBM((rows, width), BF16),
            ],
            in_specs=[whole()] * 10 + ([whole(), far()] if part else []),
            out_specs=[whole(), far()],
            input_output_aliases={11: 1} if part else {},
            scratch_shapes=[
                VMEM((rows, group * tile), BF16),
                VMEM((group * tile, key_width), BF16),
                VMEM((rows, key_width), jnp.float32),
                VMEM((blocks, rows, tile), BF16),
                pltpu.SemaphoreType.DMA((blocks,)),
            ],
            cost_estimate=cost(2 * rows * width * key_width, 6 * rows * width),
            compiler_params=room(16),
        )

    partial_sum, half_grad = products(0, [low, high] + from_x, ())
    projected, token_grad = products(1, from_y + from_far, (partial_sum, stays(half_grad)))

    all_mine = mine + [across(v) for v in mine]
    block_grad = call(
        functools.partial(slots_kernel, slots, reach),
        counts, *all_mine,
        out_shape=many(slots),
        in_specs=[scalars()] + [whole()] * (2 * INNER),
        out_specs=whole(),
        cost_estimate=cost(16 * block_bytes, 32 * block_bytes),
        compiler_params=room(8),
    )
    return (projected, token_grad, block_grad)


def solution(mesh):
    return jax.shard_map(
        body,
        mesh=mesh,
        in_specs=(
            P(("dp", "fsdp"), None),
            P("fsdp", None, None),
            P("fsdp"),
            P(),
            P(("dp", "fsdp"), None),
        ),
        out_specs=(P(("dp", "fsdp"), None), P(("dp", "fsdp"), None), P("fsdp", None, None)),
        check_vma=False,
    )
```

```python
import functools
import math

import jax
import jax.numpy as jnp
from jax import lax
from jax.experimental import pallas as pl
from jax.experimental.pallas import tpu as pltpu
from jax.sharding import PartitionSpec as P


PERIOD = 8
INNER = 4
VMEM = pltpu.VMEM
BF16 = jnp.bfloat16


def class_of(core, place):
    return (place // 2) * 4 + core * 2 + place % 2


def prefix(counts, stop):
    return lax.fori_loop(0, stop, lambda i, total: total + counts[i], jnp.int32(0))


def lead(cls, start):
    return (cls - start) & (PERIOD - 1)


def here():
    me = lax.axis_index("fsdp")
    return lax.axis_index("dp"), me // INNER, me % INNER, me


def spread_kernel(slots, reach, counts_in, scales_in, codes_in, *refs):
    (tokens_in, cot_in), (tokens, cot), outs = refs[:2], refs[2:4], refs[4 : 4 + INNER]
    counts, scales, codes, done, wide_done = refs[4 + INNER :]
    wide_loads = [
        pltpu.make_async_copy(source, target, wide_done.at[n])
        for n, (source, target) in enumerate(((tokens_in, tokens), (cot_in, cot)))
    ]
    loads = [
        pltpu.make_async_copy(source, target, done.at[n])
        for n, (source, target) in enumerate(
            ((counts_in, counts), (scales_in, scales), (codes_in, codes))
        )
    ]
    for load in loads + wide_loads:
        load.start()
    core, _, place, me = here()
    loads[0].wait()
    start = prefix(counts, me)
    loads[1].wait()
    loads[2].wait()
    for step, out in enumerate(outs):
        first = lead(class_of(core, place ^ step), start)
        for t in range(reach):
            slot = jnp.minimum(first + PERIOD * t, slots - 1)
            out[t] = (codes[slot].astype(jnp.float32) * scales[slot]).astype(BF16)
    for load in wide_loads:
        load.wait()


def stack_kernel(reach, *refs):
    out = refs[-1]
    for m, ref in enumerate(refs[:-1]):
        out[pl.ds(m * reach, reach)] = ref[...]


def class_kernel(planes, reach, counts, *refs):
    ins, outs, starts = refs[:planes], refs[planes:-1], refs[-1]
    core, plane, place, _ = here()
    cls = class_of(core, place)
    per_out = outs[0].shape[0]

    def note(i, total):
        starts[i] = total
        return total + counts[i]

    lax.fori_loop(0, planes * INNER, note, jnp.int32(0))
    for shift, ref in enumerate(ins):
        source = plane ^ shift
        for m in range(INNER):
            owner = source * INNER + (place ^ m)
            first = lead(cls, starts[owner])
            for t in range(reach):
                j = (starts[owner] + first) // PERIOD + t
                held = first + PERIOD * t < counts[owner]
                for n, out in enumerate(outs):

                    @pl.when(held & (j // per_out == n))
                    def _(j=j, t=t, m=m, n=n, ref=ref, out=out):
                        out[j - n * per_out] = ref[m * reach + t]


def grad_kernel(scale, tile, chunks, mine, theirs, cot_mine, cot_theirs, own, *refs):
    outs, quad = refs[:-1], refs[-1]
    core, _, place, _ = here()
    half = cot_mine.shape[1] // 2
    columns = pl.ds(pl.multiple_of(core * half, half), half)
    left, right = cot_mine[:, columns], cot_theirs[:, columns]
    wide = mine.shape[1] // chunks
    per_chunk = wide // (2 * tile)
    dims = (((0,), (0,)), ((), ()))

    def chunk(part, i, carry):
        base = i * per_chunk - part * (chunks // 2) * per_chunk
        for k in range(per_chunk):
            rows = pl.ds(pl.multiple_of(i * wide + 2 * tile * k, 2 * tile), 2 * tile)
            value = lax.dot_general(mine[:, rows], left, dims, preferred_element_type=jnp.float32)
            value += lax.dot_general(
                theirs[:, rows], right, dims, preferred_element_type=jnp.float32
            )
            quad[k] = value * scale
            for m in range(INNER):
                where = place ^ m
                row = pl.multiple_of((where // 2) * tile, tile)
                col = pl.multiple_of((where % 2) * tile, tile)
                block = quad[k, pl.ds(row, tile), pl.ds(col, tile)].astype(BF16)
                if m:
                    outs[2 * (m - 1) + part][base + k] = block
                else:
                    own[i * per_chunk + k] = block
        return carry

    for part in range(2):
        first = part * (chunks // 2)
        lax.fori_loop(first, first + chunks // 2, functools.partial(chunk, part), 0)


def fold_kernel(*refs):
    ins, outs = refs[: 2 * len(refs) // 3], refs[2 * len(refs) // 3 :]
    for n, out in enumerate(outs):
        value = ins[2 * n][...].astype(jnp.float32) + ins[2 * n + 1][...].astype(jnp.float32)
        out[...] = value.astype(BF16)


def window(counts, cls, plane, blocks, span):
    start = prefix(counts, plane * INNER)
    return jnp.minimum((start + lead(cls, start)) // PERIOD, blocks - span)


def plane_sum_kernel(span, counts, own, *refs):
    ins, outs, total = refs[:4], refs[4:-1], refs[-1]
    core, plane, place, _ = here()
    cls = class_of(core, place)
    blocks = total.shape[0]
    for j in range(blocks):
        part, row = divmod(j, blocks // 2)
        acc = own[j].astype(jnp.float32)
        for ref in ins[2 * part : 2 * part + 2]:
            acc += ref[row].astype(jnp.float32)
        total[j] = acc.astype(BF16)
    for shift, out in enumerate(outs):
        target = plane ^ shift
        out[...] = total[pl.ds(window(counts, cls, target, blocks, span), span)]


def owner_kernel(blocks, reach, span, counts, *refs):
    ins, outs, total = refs[: -INNER - 1], refs[-INNER - 1 : -1], refs[-1]
    core, plane, place, _ = here()
    cls = class_of(core, place)
    acc = ins[0][...].astype(jnp.float32)
    for ref in ins[1:]:
        acc += ref[...].astype(jnp.float32)
    total[...] = acc.astype(BF16)
    base = window(counts, cls, plane, blocks, span)
    for m, out in enumerate(outs):
        start = prefix(counts, plane * INNER + (place ^ m))
        j = (start + lead(cls, start)) // PERIOD - base
        for t in range(reach):
            out[t] = total[jnp.clip(j + t, 0, span - 1)]


def slots_kernel(slots, reach, counts, *refs):
    ins, out = refs[:-1], refs[-1]
    core, _, place, me = here()
    start, count = prefix(counts, me), counts[me]
    for n, ref in enumerate(ins):
        side = core ^ (n // INNER)
        first = lead(class_of(side, place ^ (n % INNER)), start)
        for t in range(reach):
            slot = first + PERIOD * t

            @pl.when(slot < slots)
            def _(slot=slot, ref=ref, t=t):
                value = ref[t]
                out[slot] = jnp.where(slot < count, value, jnp.zeros_like(value))


def product_kernel(tile, part, tokens, cot, *refs):
    pieces, refs = refs[:8], refs[8:]
    before, refs = (refs[0], refs[2:]) if part else (None, refs)
    projected, token_grad, left, weight, acc, stripes, done = refs
    core, _, place, _ = here()
    parity = (place // 2) ^ part
    per_piece = pieces[0].shape[0]
    group = left.shape[1] // tile
    stores = []
    for start in range(0, 2 * per_piece, group):
        half, first = divmod(start, per_piece)
        for k in range(group):
            lane = pl.multiple_of((2 * (start + k) + parity) * tile, tile)
            left[:, pl.ds(k * tile, tile)] = tokens[:, pl.ds(lane, tile)]
            for n in range(4):
                side, m = divmod(n, 2)
                col = pl.multiple_of(((core ^ side) * 2 + (place ^ m) % 2) * tile, tile)
                weight[pl.ds(k * tile, tile), pl.ds(col, tile)] = pieces[2 * n + half][first + k]
        value = jnp.dot(left[...], weight[...], preferred_element_type=jnp.float32)
        if start:
            acc[...] += value
        else:
            acc[...] = before[...] + value if part else value
        grads = lax.dot_general(
            cot[...], weight[...], (((1,), (1,)), ((), ())), preferred_element_type=jnp.float32
        ).astype(BF16)
        for k in range(group):
            j = start + k
            stripes[j] = grads[:, k * tile : (k + 1) * tile]
            lane = pl.multiple_of((2 * j + parity) * tile, tile)
            store = pltpu.make_async_copy(
                stripes.at[j], token_grad.at[:, pl.ds(lane, tile)], done.at[j]
            )
            store.start()
            stores.append(store)
    projected[...] = acc[...].astype(projected.dtype)
    for store in stores:
        store.wait()


def whole():
    return pl.BlockSpec(memory_space=VMEM)


def far():
    return pl.BlockSpec(memory_space=pl.ANY)


def stays(value):
    return pltpu.with_memory_space_constraint(value, pltpu.HBM)


def scalars():
    return pl.BlockSpec(memory_space=pltpu.SMEM)


def room(mebibytes):
    return pltpu.CompilerParams(vmem_limit_bytes=mebibytes * 2**20)


def cost(flops, nbytes):
    return pl.CostEstimate(flops=flops, bytes_accessed=nbytes, transcendentals=0)


def body(tokens, block_codes, scales, counts, cotangent):
    owners = lax.axis_size("fsdp")
    planes = owners // INNER
    slots, tile = block_codes.shape[:2]
    rows, width = tokens.shape
    key_width = cotangent.shape[1]
    blocks = (width // tile) * (key_width // tile) // PERIOD
    reach = -(-slots // PERIOD)
    span = min(-(-slots * INNER // PERIOD), blocks)
    total_tokens = rows * lax.axis_size("dp") * owners

    def many(n):
        return jax.ShapeDtypeStruct((n, tile, tile), BF16)

    block_bytes = tile * tile * 2

    def beside(value, m):
        return lax.ppermute(value, "fsdp", [(i, i ^ m) for i in range(owners)])

    def along(value, shift):
        pairs = [(i, i ^ (shift * INNER)) for i in range(owners)]
        return lax.ppermute(value, "fsdp", pairs)

    def across(value):
        return lax.ppermute(value, "dp", [(0, 1), (1, 0)])

    def call(kernel, *operands, **how):
        return pl.pallas_call(kernel, **how)(*operands)

    their_tokens, their_cot = across(tokens), across(cotangent)

    my_tokens, my_cot, *spread = call(
        functools.partial(spread_kernel, slots, reach),
        stays(counts),
        stays(scales),
        stays(block_codes),
        stays(tokens),
        stays(cotangent),
        out_shape=[
            pltpu.VMEM((rows, width), BF16),
            pltpu.VMEM((rows, key_width), BF16),
        ]
        + [many(reach)] * INNER,
        in_specs=[far()] * 5,
        out_specs=[far()] * 2 + [whole()] * INNER,
        scratch_shapes=[
            pltpu.SMEM((owners,), jnp.int32),
            pltpu.SMEM((slots,), jnp.float32),
            VMEM((slots, tile, tile), BF16),
            pltpu.SemaphoreType.DMA((3,)),
            pltpu.SemaphoreType.DMA((2,)),
        ],
        cost_estimate=cost(8 * block_bytes, 24 * block_bytes),
        compiler_params=room(8),
    )
    near = [spread[0]] + [beside(spread[m], m) for m in range(1, INNER)]

    chunks = 4
    half = many(blocks // 2)
    grads = call(
        functools.partial(grad_kernel, 1.0 / math.sqrt(total_tokens), tile, chunks),
        my_tokens,
        their_tokens,
        my_cot,
        their_cot,
        out_shape=[many(blocks)] + [half] * 6,
        in_specs=[whole()] * 4,
        out_specs=[whole()] * 7,
        scratch_shapes=[
            VMEM((width // (2 * tile * chunks), 2 * tile, 2 * tile), jnp.float32)
        ],
        cost_estimate=cost(2 * rows * width * key_width, 6 * rows * width),
        compiler_params=room(20),
    )
    own_part, x_low, x_high, y_low, y_high, far_low, far_high = grads
    folded = call(
        fold_kernel,
        y_low,
        beside(far_low, 1),
        x_high,
        beside(far_high, 2),
        out_shape=[half] * 2,
        in_specs=[whole()] * 4,
        out_specs=[whole()] * 2,
        cost_estimate=cost(16 * block_bytes, 48 * block_bytes),
        compiler_params=room(8),
    )
    parts = [
        own_part,
        beside(x_low, 1),
        beside(folded[0], 2),
        beside(folded[1], 1),
        beside(y_high, 2),
    ]

    stacked = call(
        functools.partial(stack_kernel, reach),
        *near,
        out_shape=many(INNER * reach),
        in_specs=[whole()] * INNER,
        out_specs=whole(),
        cost_estimate=cost(8 * block_bytes, 16 * block_bytes),
        compiler_params=room(8),
    )
    held = [stacked] + [along(stacked, s) for s in range(1, planes) if (s, planes) != (2, 4)]
    if planes == 4:
        held.insert(2, along(held[2], 1))

    own_classes = call(
        functools.partial(class_kernel, planes, reach),
        counts,
        *held,
        out_shape=[many(blocks // 2)] * 2,
        in_specs=[scalars()] + [whole()] * planes,
        out_specs=[whole()] * 2,
        scratch_shapes=[pltpu.SMEM((owners,), jnp.int32)],
        cost_estimate=cost(32 * block_bytes, 48 * block_bytes),
        compiler_params=room(8),
    )

    windows = call(
        functools.partial(plane_sum_kernel, span),
        counts, *parts,
        out_shape=[many(span)] * planes,
        in_specs=[scalars()] + [whole()] * 5,
        out_specs=[whole()] * planes,
        scratch_shapes=[VMEM((blocks, tile, tile), BF16)],
        cost_estimate=cost(64 * block_bytes, 96 * block_bytes),
        compiler_params=room(12),
    )
    if planes == 4:
        through = call(
            fold_kernel,
            windows[3],
            along(windows[2], 1),
            out_shape=[many(span)],
            in_specs=[whole()] * 2,
            out_specs=[whole()],
            cost_estimate=cost(8 * block_bytes, 24 * block_bytes),
            compiler_params=room(8),
        )
        sums = [windows[0], along(windows[1], 1), along(through[0], 3)]
    else:
        sums = [windows[0]] + [along(windows[s], s) for s in range(1, planes)]

    sent = call(
        functools.partial(owner_kernel, blocks, reach, span),
        counts, *sums,
        out_shape=[many(reach)] * INNER,
        in_specs=[scalars()] + [whole()] * len(sums),
        out_specs=[whole()] * INNER,
        scratch_shapes=[VMEM((span, tile, tile), BF16)],
        cost_estimate=cost(32 * block_bytes, 48 * block_bytes),
        compiler_params=room(8),
    )
    mine = [sent[0]] + [beside(sent[m], m) for m in range(1, INNER)]

    low, high = own_classes
    from_x = [beside(low, 1), beside(high, 1)]
    from_y = [beside(low, 2), beside(high, 2)]
    from_far = [beside(from_x[0], 2), beside(from_y[1], 1)]
    group = min(4, blocks // 2)

    def products(part, own, carried):
        held_by_both = own + [across(c) for c in own]
        return call(
            functools.partial(product_kernel, tile, part),
            my_tokens,
            my_cot,
            *held_by_both,
            *carried,
            out_shape=[
                jax.ShapeDtypeStruct((rows, key_width), BF16 if part else jnp.float32),
                pltpu.HBM((rows, width), BF16),
            ],
            in_specs=[whole()] * 10 + ([whole(), far()] if part else []),
            out_specs=[whole(), far()],
            input_output_aliases={11: 1} if part else {},
            scratch_shapes=[
                VMEM((rows, group * tile), BF16),
                VMEM((group * tile, key_width), BF16),
                VMEM((rows, key_width), jnp.float32),
                VMEM((blocks, rows, tile), BF16),
                pltpu.SemaphoreType.DMA((blocks,)),
            ],
            cost_estimate=cost(2 * rows * width * key_width, 6 * rows * width),
            compiler_params=room(16),
        )

    partial_sum, half_grad = products(0, [low, high] + from_x, ())
    projected, token_grad = products(1, from_y + from_far, (partial_sum, stays(half_grad)))

    all_mine = mine + [across(v) for v in mine]
    block_grad = call(
        functools.partial(slots_kernel, slots, reach),
        counts, *all_mine,
        out_shape=many(slots),
        in_specs=[scalars()] + [whole()] * (2 * INNER),
        out_specs=whole(),
        cost_estimate=cost(16 * block_bytes, 32 * block_bytes),
        compiler_params=room(8),
    )
    return (projected, token_grad, block_grad)


def solution(mesh):
    return jax.shard_map(
        body,
        mesh=mesh,
        in_specs=(
            P(("dp", "fsdp"), None),
            P("fsdp", None, None),
            P("fsdp"),
            P(),
            P(("dp", "fsdp"), None),
        ),
        out_specs=(P(("dp", "fsdp"), None), P(("dp", "fsdp"), None), P("fsdp", None, None)),
        check_vma=False,
    )
```

```python
import functools
import math

import jax
import jax.numpy as jnp
from jax import lax
from jax.experimental import pallas as pl
from jax.experimental.pallas import tpu as pltpu
from jax.sharding import PartitionSpec as P


PERIOD = 8
INNER = 4
VMEM = pltpu.VMEM
BF16 = jnp.bfloat16


def class_of(core, place):
    return (place // 2) * 4 + core * 2 + place % 2


def lead(cls, start):
    return (cls - start) & (PERIOD - 1)


def here():
    me = lax.axis_index("fsdp")
    return lax.axis_index("dp"), me // INNER, me % INNER, me


def spread_kernel(slots, reach, counts_in, scales_in, codes_in, *refs):
    tokens_in, cot_in, tokens, cot = refs[:4]
    outs = refs[4 : 4 + INNER]
    counts, scales, codes, done, wide_done = refs[4 + INNER :]
    wide_loads = [
        pltpu.make_async_copy(source, target, wide_done.at[n])
        for n, (source, target) in enumerate(((tokens_in, tokens), (cot_in, cot)))
    ]
    loads = [
        pltpu.make_async_copy(source, target, done.at[n])
        for n, (source, target) in enumerate(
            ((counts_in, counts), (scales_in, scales), (codes_in, codes))
        )
    ]
    for load in loads + wide_loads:
        load.start()
    core, _, place, me = here()
    loads[0].wait()
    start = lax.fori_loop(0, me, lambda i, total: total + counts[i], jnp.int32(0))
    loads[1].wait()
    loads[2].wait()
    for step, out in enumerate(outs):
        first = lead(class_of(core, place ^ step), start)
        for t in range(reach):
            slot = jnp.minimum(first + PERIOD * t, slots - 1)
            out[t] = (codes[slot].astype(jnp.float32) * scales[slot]).astype(BF16)
    for load in wide_loads:
        load.wait()


def table_kernel(owners, counts, table):
    def note(i, total):
        table[i] = total
        table[owners + i] = counts[i]
        return total + counts[i]

    lax.fori_loop(0, owners, note, jnp.int32(0), unroll=owners <= 16)


def stack_kernel(reach, *refs):
    out = refs[-1]
    for m, ref in enumerate(refs[:-1]):
        out[pl.ds(m * reach, reach)] = ref[...]


def class_kernel(planes, reach, table, *refs):
    ins, outs, gathered = refs[:planes], refs[planes:-1], refs[-1]
    core, plane, place, _ = here()
    cls = class_of(core, place)
    owners = planes * INNER
    for shift, ref in enumerate(ins):
        for m in range(INNER):
            owner = (plane ^ shift) * INNER + (place ^ m)
            start, count = table[owner], table[owners + owner]
            first = lead(cls, start)
            for t in range(reach):

                @pl.when(first + PERIOD * t < count)
                def _(start=start, first=first, t=t, m=m, ref=ref):
                    gathered[(start + first) // PERIOD + t] = ref[m * reach + t]

    per_out = outs[0].shape[0]
    for n, out in enumerate(outs):
        out[...] = gathered[n * per_out : (n + 1) * per_out]


def grad_kernel(scale, tile, chunks, mine, theirs, cot_mine, cot_theirs, own, *refs):
    outs, quad = refs[:-1], refs[-1]
    core, _, place, _ = here()
    half = cot_mine.shape[1] // 2
    columns = pl.ds(pl.multiple_of(core * half, half), half)
    left, right = cot_mine[:, columns], cot_theirs[:, columns]
    wide = mine.shape[1] // chunks
    per_chunk = wide // (2 * tile)
    dims = (((0,), (0,)), ((), ()))

    def chunk(part, i, carry):
        base = i * per_chunk - part * (chunks // 2) * per_chunk
        for k in range(per_chunk):
            rows = pl.ds(pl.multiple_of(i * wide + 2 * tile * k, 2 * tile), 2 * tile)
            value = lax.dot_general(mine[:, rows], left, dims, preferred_element_type=jnp.float32)
            value += lax.dot_general(
                theirs[:, rows], right, dims, preferred_element_type=jnp.float32
            )
            quad[k] = value * scale
            for m in range(INNER):
                where = place ^ m
                row = pl.multiple_of((where // 2) * tile, tile)
                col = pl.multiple_of((where % 2) * tile, tile)
                block = quad[k, pl.ds(row, tile), pl.ds(col, tile)].astype(BF16)
                if m:
                    outs[2 * (m - 1) + part][base + k] = block
                else:
                    own[i * per_chunk + k] = block
        return carry

    for part in range(2):
        first = part * (chunks // 2)
        lax.fori_loop(first, first + chunks // 2, functools.partial(chunk, part), 0)


def fold_kernel(*refs):
    ins, outs = refs[: 2 * len(refs) // 3], refs[2 * len(refs) // 3 :]
    for n, out in enumerate(outs):
        value = ins[2 * n][...].astype(jnp.float32) + ins[2 * n + 1][...].astype(jnp.float32)
        out[...] = value.astype(BF16)


def window(table, cls, plane, blocks, span):
    start = table[plane * INNER]
    return jnp.minimum((start + lead(cls, start)) // PERIOD, blocks - span)


def plane_sum_kernel(span, table, own, *refs):
    ins, outs, total = refs[:4], refs[4:-1], refs[-1]
    core, plane, place, _ = here()
    cls = class_of(core, place)
    blocks = total.shape[0]
    for j in range(blocks):
        part, row = divmod(j, blocks // 2)
        acc = own[j].astype(jnp.float32)
        for ref in ins[2 * part : 2 * part + 2]:
            acc += ref[row].astype(jnp.float32)
        total[j] = acc.astype(BF16)
    for shift, out in enumerate(outs):
        target = plane ^ shift
        out[...] = total[pl.ds(window(table, cls, target, blocks, span), span)]


def owner_kernel(blocks, reach, span, table, *refs):
    ins, outs = refs[:-INNER], refs[-INNER:]
    core, plane, place, _ = here()
    cls = class_of(core, place)
    base = window(table, cls, plane, blocks, span)
    for m, out in enumerate(outs):
        start = table[plane * INNER + (place ^ m)]
        j = (start + lead(cls, start)) // PERIOD - base
        for t in range(reach):
            row = jnp.clip(j + t, 0, span - 1)
            acc = ins[0][row].astype(jnp.float32)
            for ref in ins[1:]:
                acc += ref[row].astype(jnp.float32)
            out[t] = acc.astype(BF16)


def slots_kernel(slots, reach, owners, table, *refs):
    ins, (out, empty, done) = refs[:-3], refs[-3:]
    core, _, place, me = here()
    start, count = table[me], table[owners + me]
    empty[...] = jnp.zeros_like(empty)
    stores = []
    for n, ref in enumerate(ins):
        side = core ^ (n // INNER)
        first = lead(class_of(side, place ^ (n % INNER)), start)
        for t in range(reach):
            slot = first + PERIOD * t
            here_slot = jnp.minimum(slot, slots - 1)
            flag = done.at[n * reach + t]
            real = pltpu.make_async_copy(ref.at[t], out.at[here_slot], flag)
            blank = pltpu.make_async_copy(empty, out.at[here_slot], flag)
            pl.when((slot < slots) & (slot < count))(real.start)
            pl.when((slot < slots) & (slot >= count))(blank.start)
            stores.append((slot < slots, real))
    for wanted, store in stores:
        pl.when(wanted)(store.wait)


def product_kernel(tile, part, tokens, cot, *refs):
    pieces, refs = refs[:8], refs[8:]
    before, refs = (refs[0], refs[2:]) if part else (None, refs)
    projected, token_grad, left, weight, acc, stripes, done = refs
    core, _, place, _ = here()
    parity = (place // 2) ^ part
    per_piece = pieces[0].shape[0]
    group = left.shape[1] // tile
    stores = []
    for start in range(0, 2 * per_piece, group):
        half, first = divmod(start, per_piece)
        for k in range(group):
            lane = pl.multiple_of((2 * (start + k) + parity) * tile, tile)
            left[:, pl.ds(k * tile, tile)] = tokens[:, pl.ds(lane, tile)]
            for n in range(4):
                side, m = divmod(n, 2)
                col = pl.multiple_of(((core ^ side) * 2 + (place ^ m) % 2) * tile, tile)
                weight[pl.ds(k * tile, tile), pl.ds(col, tile)] = pieces[2 * n + half][first + k]
        value = jnp.dot(left[...], weight[...], preferred_element_type=jnp.float32)
        if start:
            acc[...] += value
        else:
            acc[...] = before[...] + value if part else value
        grads = lax.dot_general(
            cot[...], weight[...], (((1,), (1,)), ((), ())), preferred_element_type=jnp.float32
        ).astype(BF16)
        for k in range(group):
            j = start + k
            stripes[j] = grads[:, k * tile : (k + 1) * tile]
            lane = pl.multiple_of((2 * j + parity) * tile, tile)
            store = pltpu.make_async_copy(
                stripes.at[j], token_grad.at[:, pl.ds(lane, tile)], done.at[j]
            )
            store.start()
            stores.append(store)
    projected[...] = acc[...].astype(projected.dtype)
    for store in stores:
        store.wait()


def whole():
    return pl.BlockSpec(memory_space=VMEM)


def far():
    return pl.BlockSpec(memory_space=pl.ANY)


def stays(value):
    return pltpu.with_memory_space_constraint(value, pltpu.HBM)


def scalars():
    return pl.BlockSpec(memory_space=pltpu.SMEM)


def room(mebibytes):
    return pltpu.CompilerParams(vmem_limit_bytes=mebibytes * 2**20)


def cost(flops, nbytes):
    return pl.CostEstimate(flops=flops, bytes_accessed=nbytes, transcendentals=0)


def body(tokens, block_codes, scales, counts, cotangent):
    owners = lax.axis_size("fsdp")
    planes = owners // INNER
    slots, tile = block_codes.shape[:2]
    rows, width = tokens.shape
    key_width = cotangent.shape[1]
    blocks = (width // tile) * (key_width // tile) // PERIOD
    reach = -(-slots // PERIOD)
    span = min(-(-slots * INNER // PERIOD), blocks)
    total_tokens = rows * lax.axis_size("dp") * owners

    def many(n):
        return jax.ShapeDtypeStruct((n, tile, tile), BF16)

    block_bytes = tile * tile * 2

    def beside(value, m):
        return lax.ppermute(value, "fsdp", [(i, i ^ m) for i in range(owners)])

    def along(value, shift):
        pairs = [(i, i ^ (shift * INNER)) for i in range(owners)]
        return lax.ppermute(value, "fsdp", pairs)

    def across(value):
        return lax.ppermute(value, "dp", [(0, 1), (1, 0)])

    def call(kernel, *operands, **how):
        return pl.pallas_call(kernel, **how)(*operands)

    their_tokens, their_cot = across(tokens), across(cotangent)

    my_tokens, my_cot, *spread = call(
        functools.partial(spread_kernel, slots, reach),
        stays(counts),
        stays(scales),
        stays(block_codes),
        stays(tokens),
        stays(cotangent),
        out_shape=[
            pltpu.VMEM((rows, width), BF16),
            pltpu.VMEM((rows, key_width), BF16),
        ]
        + [many(reach)] * INNER,
        in_specs=[far()] * 5,
        out_specs=[far()] * 2 + [whole()] * INNER,
        scratch_shapes=[
            pltpu.SMEM((owners,), jnp.int32),
            pltpu.SMEM((slots,), jnp.float32),
            VMEM((slots, tile, tile), BF16),
            pltpu.SemaphoreType.DMA((3,)),
            pltpu.SemaphoreType.DMA((2,)),
        ],
        cost_estimate=cost(8 * block_bytes, 24 * block_bytes),
        compiler_params=room(8),
    )
    near = [spread[0]] + [beside(spread[m], m) for m in range(1, INNER)]

    chunks = 4
    half = many(blocks // 2)
    grads = call(
        functools.partial(grad_kernel, 1.0 / math.sqrt(total_tokens), tile, chunks),
        my_tokens,
        their_tokens,
        my_cot,
        their_cot,
        out_shape=[many(blocks)] + [half] * 6,
        in_specs=[whole()] * 4,
        out_specs=[whole()] * 7,
        scratch_shapes=[
            VMEM((width // (2 * tile * chunks), 2 * tile, 2 * tile), jnp.float32)
        ],
        cost_estimate=cost(2 * rows * width * key_width, 6 * rows * width),
        compiler_params=room(20),
    )
    own_part, x_low, x_high, y_low, y_high, far_low, far_high = grads
    folded = call(
        fold_kernel,
        y_low,
        beside(far_low, 1),
        x_high,
        beside(far_high, 2),
        out_shape=[half] * 2,
        in_specs=[whole()] * 4,
        out_specs=[whole()] * 2,
        cost_estimate=cost(16 * block_bytes, 48 * block_bytes),
        compiler_params=room(8),
    )
    parts = [
        own_part,
        beside(x_low, 1),
        beside(folded[0], 2),
        beside(folded[1], 1),
        beside(y_high, 2),
    ]

    table = call(
        functools.partial(table_kernel, owners),
        counts,
        out_shape=jax.ShapeDtypeStruct((2 * owners,), jnp.int32),
        in_specs=[scalars()],
        out_specs=scalars(),
        cost_estimate=cost(1000, 1000),
        compiler_params=room(1),
    )

    stacked = call(
        functools.partial(stack_kernel, reach),
        *near,
        out_shape=many(INNER * reach),
        in_specs=[whole()] * INNER,
        out_specs=whole(),
        cost_estimate=cost(8 * block_bytes, 16 * block_bytes),
        compiler_params=room(8),
    )
    held = [stacked] + [along(stacked, s) for s in range(1, planes) if (s, planes) != (2, 4)]
    if planes == 4:
        held.insert(2, along(held[2], 1))

    own_classes = call(
        functools.partial(class_kernel, planes, reach),
        table,
        *held,
        out_shape=[many(blocks // 2)] * 2,
        in_specs=[scalars()] + [whole()] * planes,
        out_specs=[whole()] * 2,
        scratch_shapes=[VMEM((blocks, tile, tile), BF16)],
        cost_estimate=cost(32 * block_bytes, 48 * block_bytes),
        compiler_params=room(8),
    )

    windows = call(
        functools.partial(plane_sum_kernel, span),
        table,
        *parts,
        out_shape=[many(span)] * planes,
        in_specs=[scalars()] + [whole()] * 5,
        out_specs=[whole()] * planes,
        scratch_shapes=[VMEM((blocks, tile, tile), BF16)],
        cost_estimate=cost(64 * block_bytes, 96 * block_bytes),
        compiler_params=room(12),
    )
    if planes == 4:
        through = call(
            fold_kernel,
            windows[3],
            along(windows[2], 1),
            out_shape=[many(span)],
            in_specs=[whole()] * 2,
            out_specs=[whole()],
            cost_estimate=cost(8 * block_bytes, 24 * block_bytes),
            compiler_params=room(8),
        )
        sums = [windows[0], along(windows[1], 1), along(through[0], 3)]
    else:
        sums = [windows[0]] + [along(windows[s], s) for s in range(1, planes)]

    sent = call(
        functools.partial(owner_kernel, blocks, reach, span),
        table,
        *sums,
        out_shape=[many(reach)] * INNER,
        in_specs=[scalars()] + [whole()] * len(sums),
        out_specs=[whole()] * INNER,
        cost_estimate=cost(32 * block_bytes, 48 * block_bytes),
        compiler_params=room(8),
    )
    mine = [sent[0]] + [beside(sent[m], m) for m in range(1, INNER)]

    low, high = own_classes
    from_x = [beside(low, 1), beside(high, 1)]
    from_y = [beside(low, 2), beside(high, 2)]
    from_far = [beside(from_x[0], 2), beside(from_y[1], 1)]
    group = min(2, blocks // 2)

    def products(part, own, carried):
        held_by_both = own + [across(c) for c in own]
        return call(
            functools.partial(product_kernel, tile, part),
            my_tokens,
            my_cot,
            *held_by_both,
            *carried,
            out_shape=[
                jax.ShapeDtypeStruct((rows, key_width), BF16 if part else jnp.float32),
                pltpu.HBM((rows, width), BF16),
            ],
            in_specs=[whole()] * 10 + ([whole(), far()] if part else []),
            out_specs=[whole(), far()],
            input_output_aliases={11: 1} if part else {},
            scratch_shapes=[
                VMEM((rows, group * tile), BF16),
                VMEM((group * tile, key_width), BF16),
                VMEM((rows, key_width), jnp.float32),
                VMEM((blocks, rows, tile), BF16),
                pltpu.SemaphoreType.DMA((blocks,)),
            ],
            cost_estimate=cost(2 * rows * width * key_width, 6 * rows * width),
            compiler_params=room(16),
        )

    partial_sum, half_grad = products(0, [low, high] + from_x, ())
    projected, token_grad = products(1, from_y + from_far, (partial_sum, stays(half_grad)))

    all_mine = mine + [across(v) for v in mine]
    block_grad = call(
        functools.partial(slots_kernel, slots, reach, owners),
        table,
        *all_mine,
        out_shape=many(slots),
        in_specs=[scalars()] + [whole()] * (2 * INNER),
        out_specs=far(),
        scratch_shapes=[
            VMEM((tile, tile), BF16),
            pltpu.SemaphoreType.DMA((2 * INNER * reach,)),
        ],
        cost_estimate=cost(16 * block_bytes, 32 * block_bytes),
        compiler_params=room(8),
    )
    return (projected, token_grad, block_grad)


def solution(mesh):
    return jax.shard_map(
        body,
        mesh=mesh,
        in_specs=(
            P(("dp", "fsdp"), None),
            P("fsdp", None, None),
            P("fsdp"),
            P(),
            P(("dp", "fsdp"), None),
        ),
        out_specs=(P(("dp", "fsdp"), None), P(("dp", "fsdp"), None), P("fsdp", None, None)),
        check_vma=False,
    )
```
